64 devices in a mesh: dp: 4 (over x, y), ep: 16 (over z, core).
Axes of the slice: x: 2, y: 2, z: 8, core: 2. Of those that a mesh axis runs over, the one named last changes fastest.
The devices are a block of a 4x4x8 slice.
Arguments:
- hidden: bfloat16 [512, 1280], P(('dp', 'ep')), parts along dimension 0
- topk_idx: int32 [512, 6], P(('dp', 'ep')), parts along dimension 0
- w_router: bfloat16 [1280, 64], replicated
- w_gate: bfloat16 [64, 1280, 896], P('ep')
- w_up: bfloat16 [64, 1280, 896], P('ep')
- w_down: bfloat16 [64, 896, 1280], P('ep')
- shared_gate: bfloat16 [1280, 1792], replicated
- shared_up: bfloat16 [1280, 1792], replicated
- shared_down: bfloat16 [1792, 1280], replicated
Outputs:
- output: bfloat16 [512, 1280], P(('dp', 'ep')), parts along dimension 0
There are 4 independent parts. The reference program is written for one: setup_inputs(seed, part) draws one part's arguments, and reference() takes and returns one part's arrays. A program takes and returns all parts, laid end to end along the dimension named above; an argument that names none is the same for every part.
All inputs are finite; a program needn't handle non-finite values.
Results may differ from the reference program's by a relative error of at most 0.00646848.
Values are sent between devices in bfloat16 or wider.
A program may use at most 768 MiB of HBM per device.

```python
import jax
import jax.numpy as jnp
from jax import lax

HIDDEN = 1280
EXPERTS = 64
EXPERT_FF = 896
TOP_K = 6
SHARED_FF = 1792
DEV_LIMIT = 3
GROUP_SIZE = 16
TOK_DEV = 8
GATE_SCALE = 16.0
GROUP_BATCH = GROUP_SIZE * TOK_DEV
LOCAL_EXPERTS = EXPERTS // GROUP_SIZE
ROW_TILE = 4 * 8
NUM_TILES = (GROUP_BATCH * TOP_K + ROW_TILE - 1) // ROW_TILE + EXPERTS


def draw_routing(key):
    key_hot, key_dev, key_first, key_rest = jax.random.split(key, 4)
    dev_ids = jnp.arange(GROUP_SIZE, dtype=jnp.int32)
    hot_dev = jax.random.randint(key_hot, (), 0, GROUP_SIZE)
    hot_bonus = jnp.where(dev_ids == hot_dev, 2 * GROUP_SIZE, 0)
    dev_score = jax.random.randint(key_dev, (GROUP_BATCH, GROUP_SIZE), 0, 4 * GROUP_SIZE) + hot_bonus[None, :]
    chosen_dev = lax.top_k(dev_score * GROUP_SIZE + dev_ids[None, :], DEV_LIMIT)[1]
    pool_size = DEV_LIMIT * LOCAL_EXPERTS
    pool_ids = jnp.arange(pool_size, dtype=jnp.int32)
    first_local = jax.random.randint(key_first, (GROUP_BATCH, DEV_LIMIT), 0, LOCAL_EXPERTS)
    first_slot = jnp.arange(DEV_LIMIT, dtype=jnp.int32)[None, :] * LOCAL_EXPERTS + first_local
    first_taken = jnp.any(pool_ids[None, None, :] == first_slot[:, :, None], axis=1)
    rest_score = jax.random.randint(key_rest, (GROUP_BATCH, pool_size), 0, 1 << 16) * pool_size + pool_ids[None, :]
    rest_slot = lax.top_k(jnp.where(first_taken, -1, rest_score), TOP_K - DEV_LIMIT)[1]
    all_slot = jnp.concatenate([first_slot, rest_slot], axis=1)
    slot_dev = jnp.take_along_axis(chosen_dev, all_slot // LOCAL_EXPERTS, axis=1)
    return (slot_dev * LOCAL_EXPERTS + all_slot % LOCAL_EXPERTS).astype(jnp.int32)


def normal_weight(key, shape, fan_in):
    return (jax.random.normal(key, shape, jnp.float32) * fan_in ** -0.5).astype(jnp.bfloat16)


def setup_inputs(seed: int = 0, part: int = 0) -> dict:
    key = jax.random.key(seed)
    part_key = jax.random.fold_in(key, part)
    key_hidden, key_route = jax.random.split(part_key)
    weight_keys = jax.random.split(jax.random.key(seed + 1), 7)
    hidden = jax.random.normal(key_hidden, (GROUP_BATCH, HIDDEN), jnp.float32).astype(jnp.bfloat16)
    return {
        'hidden': hidden,
        'topk_idx': draw_routing(key_route),
        'w_router': normal_weight(weight_keys[0], (HIDDEN, EXPERTS), HIDDEN),
        'w_gate': normal_weight(weight_keys[1], (EXPERTS, HIDDEN, EXPERT_FF), HIDDEN),
        'w_up': normal_weight(weight_keys[2], (EXPERTS, HIDDEN, EXPERT_FF), HIDDEN),
        'w_down': normal_weight(weight_keys[3], (EXPERTS, EXPERT_FF, HIDDEN), EXPERT_FF),
        'shared_gate': normal_weight(weight_keys[4], (HIDDEN, SHARED_FF), HIDDEN),
        'shared_up': normal_weight(weight_keys[5], (HIDDEN, SHARED_FF), HIDDEN),
        'shared_down': normal_weight(weight_keys[6], (SHARED_FF, HIDDEN), SHARED_FF),
    }


def swiglu(rows, gate_mat, up_mat, down_mat):
    gate_val = jnp.dot(rows, gate_mat, preferred_element_type=jnp.float32)
    up_val = jnp.dot(rows, up_mat, preferred_element_type=jnp.float32)
    inner_act = (jax.nn.silu(gate_val) * up_val).astype(jnp.bfloat16)
    return jnp.dot(inner_act, down_mat, preferred_element_type=jnp.float32)


def reference(hidden, topk_idx, w_router, w_gate, w_up, w_down, shared_gate, shared_up, shared_down):
    logits = jnp.dot(hidden, w_router, preferred_element_type=jnp.float32)
    route_prob = jax.nn.softmax(logits, axis=-1)
    gate_weight = GATE_SCALE * jnp.take_along_axis(route_prob, topk_idx, axis=1)
    num_choices = GROUP_BATCH * TOP_K
    flat_expert = topk_idx.reshape(num_choices)
    flat_token = jnp.arange(num_choices, dtype=jnp.int32) // TOP_K
    sort_order = jnp.argsort(flat_expert)
    sorted_expert = flat_expert[sort_order]
    counts = jnp.zeros((EXPERTS,), jnp.int32).at[flat_expert].add(1)
    seg_start = jnp.cumsum(counts) - counts
    tile_count = (counts + ROW_TILE - 1) // ROW_TILE
    tile_start = jnp.cumsum(tile_count) - tile_count
    row_rank = jnp.arange(num_choices, dtype=jnp.int32) - seg_start[sorted_expert]
    pad_slot = tile_start[sorted_expert] * ROW_TILE + row_rank
    padded_token = jnp.zeros((NUM_TILES * ROW_TILE,), jnp.int32).at[pad_slot].set(flat_token[sort_order])
    padded_gate = jnp.zeros((NUM_TILES * ROW_TILE,), jnp.float32).at[pad_slot].set(gate_weight.reshape(num_choices)[sort_order])
    tile_ids = jnp.arange(NUM_TILES, dtype=jnp.int32)
    tile_expert = jnp.clip(jnp.searchsorted(tile_start, tile_ids, side='right') - 1, 0, EXPERTS - 1)

    def tile_body(tile_in):
        tile_tokens, tile_gates, expert_id = tile_in
        tile_rows = jnp.take(hidden, tile_tokens, axis=0)
        tile_result = swiglu(tile_rows, w_gate[expert_id], w_up[expert_id], w_down[expert_id])
        return tile_result.astype(jnp.bfloat16).astype(jnp.float32) * tile_gates[:, None]

    tile_out = lax.map(tile_body, (padded_token.reshape(NUM_TILES, ROW_TILE), padded_gate.reshape(NUM_TILES, ROW_TILE), tile_expert))
    routed = jax.ops.segment_sum(tile_out.reshape(NUM_TILES * ROW_TILE, HIDDEN), padded_token, num_segments=GROUP_BATCH)
    shared_out = swiglu(hidden, shared_gate, shared_up, shared_down)
    return (shared_out + routed).astype(jnp.bfloat16)
```

```python
import functools

import jax
import jax.numpy as jnp
from jax import lax
from jax.experimental import pallas as pl
from jax.experimental.pallas import tpu as pltpu
from jax.sharding import PartitionSpec as P

GATE_SCALE = 16.0
MESH = pl.DeviceIdType.MESH
LANES = 128
BLOCK = 256


def silu_mul(gate_val, up_val):
    return (gate_val / (1.0 + jnp.exp(-gate_val)) * up_val).astype(jnp.bfloat16)


def dot(lhs, rhs):
    return jnp.dot(lhs, rhs, preferred_element_type=jnp.float32)


def moe_kernel(n, hidden, idx, wr, wg, wu, wd, sg, su, sd, out,
               x_buf, id_buf, wr_buf, wg_buf, wu_buf, wd_buf, sg_buf, su_buf, sd_buf,
               h_buf, hs_buf, gate_buf, part, recv,
               in_sems, w_sems, s_sems, xs_sem, xr_sem, is_sem, ir_sem, ps_sem, pr_sem):
    me = lax.axis_index('ep')
    tok_rows = hidden.shape[0]
    local_experts, hidden_dim, ff = wg.shape
    shared_blocks = sg.shape[1] // LANES
    full = ff // BLOCK * BLOCK

    barrier = pltpu.get_barrier_semaphore()
    for d in range(1, n):
        pl.semaphore_signal(barrier, inc=1, device_id={'ep': lax.rem(me + d, n)}, device_id_type=MESH)

    my_rows = pl.ds(pl.multiple_of(me * tok_rows, tok_rows), tok_rows)
    copy_x = pltpu.make_async_copy(hidden, x_buf.at[my_rows], in_sems.at[0])
    copy_i = pltpu.make_async_copy(idx, id_buf.at[my_rows], in_sems.at[1])
    copy_r = pltpu.make_async_copy(wr, wr_buf, in_sems.at[2])
    copy_x.start()
    copy_i.start()
    copy_r.start()
    shared_id = jnp.minimum(me, shared_blocks - 1)
    cols = pl.ds(pl.multiple_of(shared_id * LANES, LANES), LANES)
    copy_s = [pltpu.make_async_copy(sg.at[:, cols], sg_buf, s_sems.at[0]),
              pltpu.make_async_copy(su.at[:, cols], su_buf, s_sems.at[1]),
              pltpu.make_async_copy(sd.at[cols], sd_buf, s_sems.at[2])]
    for c in copy_s:
        c.start()
    copy_g = [pltpu.make_async_copy(wg.at[e], wg_buf.at[e], w_sems.at[0, e]) for e in range(local_experts)]
    copy_u = [pltpu.make_async_copy(wu.at[e], wu_buf.at[e], w_sems.at[1, e]) for e in range(local_experts)]
    copy_d = [pltpu.make_async_copy(wd.at[e], wd_buf.at[e], w_sems.at[2, e]) for e in range(local_experts)]
    for e in range(local_experts):
        copy_g[e].start()
        copy_u[e].start()
    for e in range(local_experts):
        copy_d[e].start()

    copy_x.wait()
    copy_i.wait()
    pl.semaphore_wait(barrier, n - 1)
    x_sends, i_sends = [], []
    for d in range(1, n):
        peer = {'ep': lax.rem(me + d, n)}
        x_sends.append(pltpu.make_async_remote_copy(
            x_buf.at[my_rows], x_buf.at[my_rows], xs_sem.at[d], xr_sem.at[d], device_id=peer, device_id_type=MESH))
        i_sends.append(pltpu.make_async_remote_copy(
            id_buf.at[my_rows], id_buf.at[my_rows], is_sem.at[d], ir_sem.at[d], device_id=peer, device_id_type=MESH))
    for c in x_sends:
        c.start()
    for c in i_sends:
        c.start()
    for c in x_sends:
        c.wait()
    for c in i_sends:
        c.wait()

    copy_r.wait()
    logits = dot(x_buf[...], wr_buf[...])
    expd = jnp.exp(logits - jnp.max(logits, axis=-1, keepdims=True))
    prob = expd / jnp.sum(expd, axis=-1, keepdims=True)
    lane_expert = lax.broadcasted_iota(jnp.int32, prob.shape, 1)
    ids = id_buf[...]
    for e in range(local_experts):
        expert = me * local_experts + e
        gate = GATE_SCALE * jnp.sum(jnp.where(lane_expert == expert, prob, 0.0), axis=-1, keepdims=True)
        hit = jnp.sum((ids == expert).astype(jnp.float32), axis=-1, keepdims=True)
        gate_buf[e] = jnp.broadcast_to(jnp.where(hit > 0.0, gate, -1.0), gate_buf.shape[1:])

    copy_s[0].wait()
    copy_s[1].wait()
    both = dot(x_buf[...], jnp.concatenate([sg_buf[...], su_buf[...]], axis=1))
    inner = silu_mul(both[:, :LANES], both[:, LANES:])
    hs_buf[...] = jnp.where(me < shared_blocks, inner, jnp.zeros_like(inner))

    for e in range(local_experts):
        copy_g[e].wait()
        copy_u[e].wait()
        for lo in range(0, full, BLOCK):
            gate_val = dot(x_buf[...], wg_buf[e, :, lo:lo + BLOCK])
            up_val = dot(x_buf[...], wu_buf[e, :, lo:lo + BLOCK])
            h_buf[e, :, lo:lo + BLOCK] = silu_mul(gate_val, up_val)
        if full < ff:
            both = dot(x_buf[...], jnp.concatenate([wg_buf[e, :, full:], wu_buf[e, :, full:]], axis=1))
            h_buf[e, :, full:] = silu_mul(both[:, :ff - full], both[:, ff - full:])

    copy_s[2].wait()
    for e in range(local_experts):
        copy_d[e].wait()
    for lo in range(0, hidden_dim, BLOCK):
        acc = dot(hs_buf[...], sd_buf[:, lo:lo + BLOCK])
        for e in range(local_experts):
            val = dot(h_buf[e], wd_buf[e, :, lo:lo + BLOCK]).astype(jnp.bfloat16).astype(jnp.float32)
            gate = jnp.concatenate([gate_buf[e]] * (BLOCK // LANES), axis=1)
            acc += jnp.where(gate >= 0.0, gate * val, 0.0)
        part[:, lo:lo + BLOCK] = acc

    p_sends = []
    for d in range(1, n):
        peer = lax.rem(me + d, n)
        rows = pl.ds(pl.multiple_of(peer * tok_rows, tok_rows), tok_rows)
        p_sends.append(pltpu.make_async_remote_copy(
            part.at[rows], recv.at[d], ps_sem.at[d], pr_sem.at[d], device_id={'ep': peer}, device_id_type=MESH))
        p_sends[-1].start()
    total = part[my_rows]
    for d, c in enumerate(p_sends, 1):
        c.wait_recv()
        total += recv[d]
    out[...] = total.astype(out.dtype)
    for c in p_sends:
        c.wait_send()


def solution(mesh):
    group_size = mesh.shape['ep']
    row_spec = P(('dp', 'ep'), None)
    expert_spec = P('ep', None, None)

    def local_moe(hidden, topk_idx, w_router, w_gate, w_up, w_down, shared_gate, shared_up, shared_down):
        tok_rows, hidden_dim = hidden.shape
        top_k = topk_idx.shape[1]
        local_experts, _, ff = w_gate.shape
        rows = tok_rows * group_size
        bf16 = jnp.bfloat16
        any_spec = pl.BlockSpec(memory_space=pl.ANY)
        dma = pltpu.SemaphoreType.DMA
        return pl.pallas_call(
            functools.partial(moe_kernel, group_size),
            out_shape=jax.ShapeDtypeStruct((tok_rows, hidden_dim), bf16),
            in_specs=[any_spec] * 9,
            out_specs=pl.BlockSpec(memory_space=pltpu.VMEM),
            scratch_shapes=[
                pltpu.VMEM((rows, hidden_dim), bf16),
                pltpu.VMEM((rows, top_k), jnp.int32),
                pltpu.VMEM(w_router.shape, bf16),
                pltpu.VMEM(w_gate.shape, bf16),
                pltpu.VMEM(w_up.shape, bf16),
                pltpu.VMEM(w_down.shape, bf16),
                pltpu.VMEM((hidden_dim, LANES), bf16),
                pltpu.VMEM((hidden_dim, LANES), bf16),
                pltpu.VMEM((LANES, hidden_dim), bf16),
                pltpu.VMEM((local_experts, rows, ff), bf16),
                pltpu.VMEM((rows, LANES), bf16),
                pltpu.VMEM((local_experts, rows, LANES), jnp.float32),
                pltpu.VMEM((rows, hidden_dim), jnp.float32),
                pltpu.VMEM((group_size, tok_rows, hidden_dim), jnp.float32),
                dma((3,)), dma((3, local_experts)), dma((3,)),
                dma((group_size,)), dma((group_size,)), dma((group_size,)), dma((group_size,)),
                dma((group_size,)), dma((group_size,)),
            ],
            compiler_params=pltpu.CompilerParams(
                collective_id=0, has_side_effects=True, vmem_limit_bytes=56 * 1024 * 1024),
            name='moe_step',
        )(hidden, topk_idx, w_router, w_gate, w_up, w_down, shared_gate, shared_up, shared_down)

    return jax.shard_map(local_moe, mesh=mesh,
                         in_specs=(row_spec, row_spec, P(), expert_spec, expert_spec, expert_spec, P(), P(), P()),
                         out_specs=row_spec, check_vma=False)
```
